32 devices in a mesh: group: 4 (over x, core), prompt: 8 (over z, y).
Axes of the slice: x: 2, y: 2, z: 4, core: 2. Of those that a mesh axis runs over, the one named last changes fastest.
Arguments:
- queries: bfloat16 [8, 4, 64, 3072], P('prompt', 'group'), may hold values from -48 to 48
- fresh_latent: bfloat16 [8, 4, 64, 576], P('prompt', 'group'), may hold values from -6 to 6
- latent_cache: bfloat16 [8, 4, 512, 576], P('prompt', 'group'), may hold values from -48 to 48
- selected: int32 [8, 4, 64], P('prompt', 'group'), may hold values from 0 to 511, as said below
- position: int32 [8, 4], P('prompt'), may hold values from 0 to 3, each once within a row
- latent_gain: bfloat16 [512], replicated, may hold values from 0.099609375 to 1.8984375
- kv_up: bfloat16 [512, 4096], P('prompt'), may hold values from -0.25 to 0.25
- out_weight: bfloat16 [2048, 2048], P('prompt'), may hold values from -0.125 to 0.125
Outputs:
- attended: bfloat16 [8, 4, 64, 2048], P('prompt', 'group')
- blended: bfloat16 [8, 4, 512, 576], P('prompt', 'group')
The draws below stay inside these ranges and needn't reach their ends.
Inputs may be any that keep to these rules, and one draw needn't show every extreme that they name: `selected`: the 64 indices of a group are distinct and increasing.
All inputs are finite; a program needn't handle non-finite values.
Results may differ from the reference program's by a relative error of at most 0.011.
Values may be sent and summed in bfloat16 or wider, within the bound.
No kernel may reach another device: no remote copies, remote signals or barrier semaphores. Data moves between devices by JAX's collectives and lax.ppermute only.
A program may use at most 128 MiB of HBM per device.

```python
import jax
import jax.numpy as jnp
from jax import lax

D = 2048
H = 16
DN = 128
DR = 64
DV = 128
LAT = 512
GROUP_LEN = 512
SEL = 64
GROUPS = 4
PROMPTS = 8


def draw_queries(key, part):
    base = jnp.clip(jax.random.normal(key, (PROMPTS, GROUPS, SEL, H, DN + DR), jnp.float32), -6.0, 6.0)
    return base.reshape(PROMPTS, GROUPS, SEL, H * (DN + DR)).astype(jnp.bfloat16)


def draw_latent_cache(key, part):
    base = jnp.clip(jax.random.normal(key, (PROMPTS, GROUPS, GROUP_LEN, LAT + DR), jnp.float32), -6.0, 6.0)
    return base.astype(jnp.bfloat16)


def draw_selected(key, part):
    raw = jax.random.randint(key, (PROMPTS, GROUPS, GROUP_LEN), 0, 1048576)
    scores = raw * GROUP_LEN + jnp.arange(GROUP_LEN, dtype=jnp.int32)
    picked = jax.lax.top_k(scores, SEL)[1]
    return jnp.sort(picked, -1).astype(jnp.int32)


def level_of(stream_key, shape, split, low, largest):
    def one(axis_at, parts):
        steps = jax.random.uniform(jax.random.fold_in(jax.random.fold_in(stream_key, 6), axis_at), (parts,), jnp.float32, low / len(split), largest / len(split))
        return jnp.repeat(jnp.exp(steps), shape[axis_at] // parts).reshape((-1,) + (1,) * (len(shape) - axis_at - 1))

    level = one(*split[0])
    for cut in split[1:]:
        level = level * one(*cut)
    return level


def scatter_about(rng, extent, width, reach, split=(), held_as=jnp.bfloat16):
    entries = jax.random.normal(rng, extent, jnp.float32) * width
    if len(split) > 0:
        entries = level_of(rng, extent, split, -0.22, 0.18) * entries
    return jnp.clip(entries, min=-reach, max=reach).astype(held_as)


def setup_inputs(seed: int = 0) -> dict:
    seeds = jax.random.split(jax.random.key(seed), 9)
    return {
        "queries": draw_queries(jax.random.fold_in(seeds[8], 71), 0),
        "fresh_latent": scatter_about(seeds[1], (PROMPTS, GROUPS, SEL, LAT + DR), 1.0, 6.0, ((0, 8), (1, 4))),
        "latent_cache": draw_latent_cache(jax.random.fold_in(seeds[8], 71), 0),
        "selected": draw_selected(jax.random.fold_in(seeds[8], 71), 0),
        "position": jax.vmap(lambda own: jax.random.permutation(own, GROUPS))(jax.random.split(seeds[4], PROMPTS)).reshape((PROMPTS, GROUPS)).astype(jnp.int32),
        "latent_gain": jnp.clip(1.0 + 0.18 * jax.random.normal(seeds[5], (LAT,), jnp.float32), 0.099609375, 1.8984375).astype(jnp.bfloat16),
        "kv_up": scatter_about(seeds[6], (LAT, H * (DN + DV)), LAT ** -0.5, 0.25, ((0, 8),)),
        "out_weight": scatter_about(seeds[7], (H * DV, D), (H * DV) ** -0.5, 0.125, ((0, 8),)),
    }


def rope_rotate(values, places):
    half = values.shape[-1] // 2
    freqs = 10000.0 ** (-jnp.arange(half, dtype=jnp.float32) / half)
    angles = places[..., None] * freqs
    cosine = jnp.cos(angles)
    sine = jnp.sin(angles)
    first = values[..., :half]
    second = values[..., half:]
    return jnp.concatenate([first * cosine - second * sine, second * cosine + first * sine], -1)

def prepare_rows(fresh, gain, places):
    latent = fresh[..., :LAT].astype(jnp.float32)
    factor = lax.rsqrt(lax.optimization_barrier(jnp.mean(latent * latent, -1, keepdims=True)) + 1e-06)
    normed = latent * factor * gain.astype(jnp.float32)
    turned = rope_rotate(fresh[..., LAT:].astype(jnp.float32), places)
    return jnp.concatenate([normed, turned], -1).astype(jnp.bfloat16)

def reference(queries, fresh_latent, latent_cache, selected, position, latent_gain, kv_up, out_weight):
    place_int = (position[:, :, None] * GROUP_LEN + selected).astype(jnp.int32)
    places = place_int.astype(jnp.float32)
    fresh_rows = prepare_rows(fresh_latent, latent_gain, places)
    prompt_ids = jnp.arange(PROMPTS, dtype=jnp.int32)[:, None, None]
    group_ids = jnp.arange(GROUPS, dtype=jnp.int32)[None, :, None]
    blended = latent_cache.at[prompt_ids, group_ids, selected].set(fresh_rows)
    weights_kv = kv_up.reshape(LAT, H, DN + DV).astype(jnp.float32)
    shaped = queries.reshape(PROMPTS, GROUPS, SEL, H, DN + DR)
    absorbed = jnp.einsum('pcshd,lhd->pcshl', shaped[..., :DN].astype(jnp.float32), weights_kv[..., :DN], precision=lax.Precision.HIGHEST).astype(jnp.bfloat16)
    turned = rope_rotate(shaped[..., DN:].astype(jnp.float32), places[..., None]).astype(jnp.bfloat16)
    query_vec = jnp.concatenate([absorbed, turned], -1).reshape(PROMPTS, GROUPS * SEL, H, LAT + DR)
    key_place = (position[:, :, None] * GROUP_LEN + jnp.arange(GROUP_LEN, dtype=jnp.int32)[None, None, :]).astype(jnp.int32)
    key_place = key_place.reshape(PROMPTS, GROUPS * GROUP_LEN)
    scale = (DN + DR) ** (-0.5)

    def one_prompt(items):
        qvec, keys, qplace, kplace = items
        scores = jnp.einsum('qhe,ke->qhk', qvec.astype(jnp.float32), keys.astype(jnp.float32), precision=lax.Precision.HIGHEST) * scale
        mask = (kplace[None, :] <= qplace[:, None])[:, None, :]
        peak = lax.optimization_barrier(jnp.max(jnp.where(mask, scores, -1e+30), -1, keepdims=True))
        probs = jnp.where(mask, jnp.exp(scores - peak), 0.0)
        total = lax.optimization_barrier(jnp.sum(probs, -1))
        rounded = lax.optimization_barrier(probs.astype(jnp.bfloat16))
        mixed = jnp.einsum('qhk,kl->qhl', rounded.astype(jnp.float32), keys[:, :LAT].astype(jnp.float32), precision=lax.Precision.HIGHEST)
        return (mixed / total[..., None]).astype(jnp.bfloat16)
    latent_mix = lax.map(one_prompt, (query_vec, blended.reshape(PROMPTS, GROUPS * GROUP_LEN, LAT + DR), place_int.reshape(PROMPTS, GROUPS * SEL), key_place))
    heads = jnp.einsum('pqhl,lhv->pqhv', latent_mix.astype(jnp.float32), weights_kv[..., DN:], precision=lax.Precision.HIGHEST).astype(jnp.bfloat16)
    heads = heads.reshape(PROMPTS * GROUPS * SEL, H * DV)
    attended = jnp.dot(heads, out_weight, preferred_element_type=jnp.float32).astype(jnp.bfloat16)
    return (attended.reshape(PROMPTS, GROUPS, SEL, D), blended)
```

```python
import functools

import jax
import jax.numpy as jnp
import numpy as np
from jax import lax
from jax.experimental import pallas as pl
from jax.experimental.pallas import tpu as pltpu
from jax.sharding import PartitionSpec as P

H = 16
DN = 128
DR = 64
DV = 128
LAT = 512
ROW = LAT + DR
SELROWS = 16
LOW = 256
NEG = -1e30
F32 = jnp.float32
BF16 = jnp.bfloat16


VMEM = pl.BlockSpec(memory_space=pltpu.VMEM)
SMEM = pl.BlockSpec(memory_space=pltpu.SMEM)
ANY = pl.BlockSpec(memory_space=pl.ANY)


def iota(shape, axis):
    return lax.broadcasted_iota(jnp.int32, shape, axis)


def column_of(row):
    n = row.shape[-1]
    square = jnp.where(iota((n, n), 0) == iota((n, n), 1), jnp.broadcast_to(row, (n, n)), 0.0)
    return jnp.sum(square, -1, keepdims=True)


def rotate(tile, cosine, sine):
    lane = iota(tile.shape, 1) % DR
    other = jnp.where(lane < DR // 2, pltpu.roll(tile, 2 * DR - DR // 2, 1), pltpu.roll(tile, DR // 2, 1))
    return tile * cosine + other * sine


def prep_kernel(group_size, quad, position, selected, fresh, cache, gain, freqs, queries, *refs):
    g = lax.axis_index("group")
    per = H // group_size
    picks = fresh.shape[0]
    length = cache.shape[1]
    if quad:
        blended, far, near, far_q, own_q, q_all = refs
    else:
        blended, far, out_q, q_all = refs
    sel_row = selected[...].astype(F32)
    sel = column_of(sel_row)
    place = position[0, g].astype(F32) * length + sel
    angle = place * freqs[...]
    cosine = jnp.cos(angle)
    sine = jnp.sin(angle)
    sine = jnp.where(iota(sine.shape, 1) % DR < DR // 2, -sine, sine)

    for pair in range(H // 2):
        base = pair * 2 * (DN + DR)
        tile1 = queries[:, base + 128 : base + 256].astype(F32)
        tile2 = queries[:, base + 256 : base + 384].astype(F32)
        low = iota(tile1.shape, 1) < DR
        turned = rotate(jnp.where(low, tile1, tile2), cosine, sine)
        other = pltpu.roll(turned, DR, 1)
        second = pltpu.roll(jnp.where(low, tile2, tile1), DR, 1)
        for odd in range(2):
            head = 2 * pair + odd
            slot, r = divmod(head, group_size)
            nope = second.astype(BF16) if odd else queries[:, base : base + 128]
            q_all[r, 0:picks, slot * DN : (slot + 1) * DN] = nope
            want_high = slot % 2 == 1
            piece = (turned if (odd == 1) == want_high else other).astype(BF16)
            col = slot // 2 * 128 + (DR if want_high else 0)
            mine = piece[:, DR:] if want_high else piece[:, :DR]
            half = picks // 2
            q_all[r, picks : picks + half, col : col + DR] = mine[:half]
            q_all[r, picks : picks + half, per * DR + col : per * DR + col + DR] = mine[half:]

    latent = fresh[:, :LAT].astype(F32)
    factor = lax.rsqrt(jnp.mean(latent * latent, -1, keepdims=True) + 1e-06)
    normed = (latent * factor * gain[...].astype(F32)).astype(BF16)
    tail = fresh[:, LAT:].astype(F32)
    swapped = jnp.concatenate([tail[:, DR // 2 :], tail[:, : DR // 2]], 1)
    turned = (tail * cosine[:, :DR] + swapped * sine[:, :DR]).astype(BF16)
    hot = iota((picks, length), 1).astype(F32) == sel
    hot_bf = hot.astype(BF16)
    hit = jnp.sum(hot.astype(F32), 0, keepdims=True) > 0.5
    over_rows = (((0,), (0,)), ((), ()))
    for start, rows in ((0, normed), (LAT, turned)):
        placed = lax.dot_general(rows, hot_bf, over_rows, preferred_element_type=F32)
        stop = start + rows.shape[1]
        mixed = jnp.where(hit, placed, cache[start:stop, :].astype(F32)).astype(BF16)
        blended[start:stop, :] = mixed
        far[start:stop, :] = mixed
        if quad:
            near[start:stop, :] = mixed
    high = jnp.floor(sel_row / LOW)
    low = sel_row - high * LOW
    at = iota((SELROWS, picks), 0)
    coded = jnp.where(at == 0, low, jnp.where(at == 1, high, 0.0)).astype(BF16)
    coded = jnp.concatenate([coded, jnp.zeros((SELROWS, length - picks), BF16)], 1)
    far[ROW : ROW + SELROWS, :] = coded
    if quad:
        near[ROW : ROW + SELROWS, :] = coded
        x, c = g // 2, g % 2
        far[ROW + SELROWS :, :] = q_all[2 * (1 - c) + 1 - x]
        near[ROW + SELROWS :, :] = q_all[2 * (1 - c) + x]
        far_q[...] = q_all[2 * c + 1 - x]
        own_q[...] = q_all[2 * c + x]
    else:
        out_q[...] = q_all[...]


def prep(group_size, quad, position, selected, fresh, cache, gain, freqs, queries):
    picks = fresh.shape[0]
    length = cache.shape[1]
    per = H // group_size
    q_rows = picks + picks // 2
    width = per * DN
    keys = ROW + SELROWS
    out = [jax.ShapeDtypeStruct((ROW, length), BF16)]
    if quad:
        out += [jax.ShapeDtypeStruct((keys + q_rows, length), BF16)] * 2
        out += [jax.ShapeDtypeStruct((q_rows, width), BF16)] * 2
    else:
        out += [jax.ShapeDtypeStruct((keys, length), BF16), jax.ShapeDtypeStruct((group_size, q_rows, width), BF16)]
    return pl.pallas_call(
        functools.partial(prep_kernel, group_size, quad),
        out_shape=out,
        in_specs=[SMEM] + [VMEM] * 6,
        out_specs=[VMEM] * len(out),
        scratch_shapes=[pltpu.VMEM((group_size, q_rows, width), BF16)],
        cost_estimate=pl.CostEstimate(flops=50_000_000, bytes_accessed=4_000_000, transcendentals=0),
        name="prep",
    )(position, selected, fresh, cache, gain, freqs, queries)


def cut_kernel(group_size, quad, kv, w, k_out, v_out, *w_out):
    g = lax.axis_index("group")
    per = H // group_size
    x, c = g // 2, g % 2
    r = 2 * c + x if quad else g
    for slot in range(per):
        at = pl.multiple_of((slot * group_size + r) * (DN + DV), DN + DV)
        both = kv[:, pl.ds(at, DN + DV)]
        k_out[:, slot * DN : (slot + 1) * DN] = both[:, :DN]
        v_out[:, slot * DV : (slot + 1) * DV] = both[:, DN:]
    if quad:
        w_out[0][...] = w[pl.ds(pl.multiple_of(x * DV, DV), DV), :]


def cut(group_size, quad, kv, w):
    rows = kv.shape[0]
    width = H // group_size * DN
    out = [jax.ShapeDtypeStruct((rows, width), BF16)] * 2
    if quad:
        out += [jax.ShapeDtypeStruct((DV, w.shape[1]), BF16)]
    return pl.pallas_call(
        functools.partial(cut_kernel, group_size, quad),
        out_shape=out,
        in_specs=[VMEM] * 2,
        out_specs=[VMEM] * len(out),
        cost_estimate=pl.CostEstimate(flops=1_000_000, bytes_accessed=2_000_000, transcendentals=0),
        name="cut",
    )(kv, w)


def fill(parts, refs, target):
    for (first, start, rows), ref in zip(parts, refs):
        target[pl.ds(first, rows), :] = ref[start : start + rows, :]


def attend_kernel(group_size, n_key, n_q, key_parts, rows_of, slot_group, picks, position, *refs):
    key_refs = refs[:n_key]
    q_refs = refs[n_key : n_key + n_q]
    k_refs = refs[n_key + n_q : -8]
    mix, keys, k_up, query, picked, acc, peak, total = refs[-8:]
    slots = group_size
    per = H // group_size
    length = keys.shape[2]
    rows = per * picks
    last = (((1,), (1,)), ((), ()))
    places = [position[0, slot_group(s)] for s in range(slots)]

    fill([(pl.multiple_of(a, n), b, n) for a, b, n in rows_of()], k_refs, k_up)
    for s in range(slots):
        keys[s] = key_refs[s][0:ROW, :]
        coded = key_refs[s][ROW : ROW + SELROWS, 0:picks].astype(F32)
        sel = column_of(coded[0:1] + LOW * coded[1:2])
        q = q_refs[s]
        start = key_parts[s]
        half = picks // 2
        for j in range(per):
            picked[s, j * picks : (j + 1) * picks, :] = jnp.broadcast_to(sel, (picks, 128))
            folded = q[start + picks : start + picks + half, :]
            for k in range(2):
                at = k * per * DR + j * DR
                query[s, j * picks + k * half : j * picks + (k + 1) * half, LAT:] = folded[:, at : at + DR]
    for j in range(per):
        plain = jnp.concatenate(
            [q_refs[s][key_parts[s] : key_parts[s] + picks, j * DN : (j + 1) * DN] for s in range(slots)], 0
        )
        absorbed = lax.dot_general(plain, k_up[:, j * DN : (j + 1) * DN], last, preferred_element_type=F32)
        absorbed = absorbed.astype(BF16)
        for s in range(slots):
            query[s, j * picks : (j + 1) * picks, :LAT] = absorbed[s * picks : (s + 1) * picks]

    scale = (DN + DR) ** (-0.5) * float(np.log2(np.e))

    def one(a, _):
        place = position[0, slot_group(a)]
        q = query[a]
        s = jnp.dot(q, keys[a], preferred_element_type=F32) * scale
        allowed = iota((rows, length), 1).astype(F32) <= picked[a][:, 0:1]
        s = jnp.where(allowed, s, NEG)
        top = jnp.max(s, -1, keepdims=True)
        p = jnp.exp2(s - top)
        peak[...] = top
        total[...] = jnp.sum(p, -1, keepdims=True)
        acc[...] = lax.dot_general(p.astype(BF16), keys[a, :LAT, :], last, preferred_element_type=F32)

        def other(b, _):
            @pl.when(position[0, slot_group(b)] < place)
            def _():
                s = jnp.dot(query[a], keys[b], preferred_element_type=F32) * scale
                old = peak[...]
                top = jnp.maximum(old, jnp.max(s, -1, keepdims=True))
                decay = jnp.exp2(old - top)
                p = jnp.exp2(s - top)
                peak[...] = top
                total[...] = total[...] * decay + jnp.sum(p, -1, keepdims=True)
                acc[...] = acc[...] * decay + lax.dot_general(
                    p.astype(BF16), keys[b, :LAT, :], last, preferred_element_type=F32
                )

            return 0

        lax.fori_loop(0, slots, other, 0)
        done = (acc[...] / total[...]).astype(BF16)
        for j in range(per):
            mix[j, pl.ds(pl.multiple_of(a * picks, picks), picks), :] = done[j * picks : (j + 1) * picks]
        return 0

    lax.fori_loop(0, slots, one, 0)


def attend(group_size, picks, position, key_list, q_list, q_starts, k_list, rows_of, slot_group):
    per = H // group_size
    length = key_list[0].shape[1]
    rows = per * picks
    slots = group_size
    kernel = functools.partial(
        attend_kernel, group_size, len(key_list), len(q_list), q_starts, rows_of, slot_group, picks
    )
    return pl.pallas_call(
        kernel,
        out_shape=jax.ShapeDtypeStruct((per, slots * picks, LAT), BF16),
        in_specs=[SMEM] + [VMEM] * (len(key_list) + len(q_list) + len(k_list)),
        out_specs=VMEM,
        scratch_shapes=[
            pltpu.VMEM((slots, ROW, length), BF16),
            pltpu.VMEM((LAT, per * DN), BF16),
            pltpu.VMEM((slots, rows, ROW), BF16),
            pltpu.VMEM((slots, rows, 128), F32),
            pltpu.VMEM((rows, LAT), F32),
            pltpu.VMEM((rows, 1), F32),
            pltpu.VMEM((rows, 1), F32),
        ],
        cost_estimate=pl.CostEstimate(flops=5_000_000_000, bytes_accessed=8_000_000, transcendentals=0),
        name="attend",
    )(position, *key_list, *q_list, *k_list)


def project_kernel(group_size, n_v, v_rows_of, w_places, quad, mix, *refs):
    v_refs = refs[:n_v]
    per = H // group_size
    if quad:
        w_refs = refs[n_v : -6]
        send, keep, v_up, heads, w, sems = refs[-6:]
        which, firsts = w_places()
        n = len(w_refs) // 2

        @pl.when(which)
        def _():
            for k in range(n):
                pltpu.make_async_copy(w_refs[k], w.at[pl.ds(pl.multiple_of(firsts[k], DV), DV), :], sems.at[k]).start()

        @pl.when(jnp.logical_not(which))
        def _():
            for k in range(n):
                pltpu.make_async_copy(
                    w_refs[n + k], w.at[pl.ds(pl.multiple_of(firsts[k], DV), DV), :], sems.at[k]
                ).start()
    else:
        w = refs[n_v]
        send, v_up, heads = refs[-3:]
    fill([(pl.multiple_of(a, m), b, m) for a, b, m in v_rows_of()], v_refs, v_up)
    for j in range(per):
        up = jnp.dot(mix[j], v_up[:, j * DV : (j + 1) * DV], preferred_element_type=F32)
        heads[:, j * DV : (j + 1) * DV] = up.astype(BF16)
    if quad:
        for k in range(n):
            pltpu.make_async_copy(w_refs[k], w.at[pl.ds(pl.multiple_of(firsts[k], DV), DV), :], sems.at[k]).wait()
    width = w.shape[1]
    step = min(width, 512)
    picks = send.shape[1]
    for at in range(0, width, step):
        out = jnp.dot(heads[...], w[:, at : at + step], preferred_element_type=F32)
        for s in range(group_size):
            piece = out[s * picks : (s + 1) * picks]
            if not quad:
                send[s, :, at : at + step] = piece.astype(BF16)
            elif s % 2:
                send[s // 2, :, at : at + step] = piece.astype(BF16)
            else:
                keep[s // 2, :, at : at + step] = piece


def project(group_size, picks, mix, v_list, v_rows_of, w_list, w_places, quad):
    per = H // group_size
    width = w_list[0].shape[1]
    scratch = [pltpu.VMEM((LAT, per * DV), BF16), pltpu.VMEM((group_size * picks, per * DV), BF16)]
    if quad:
        out = [
            jax.ShapeDtypeStruct((2, picks, width), BF16),
            jax.ShapeDtypeStruct((2, picks, width), F32),
        ]
        scratch += [pltpu.VMEM((per * DV, width), BF16), pltpu.SemaphoreType.DMA((per,))]
    else:
        out = [jax.ShapeDtypeStruct((group_size, picks, width), BF16)]
    return pl.pallas_call(
        functools.partial(project_kernel, group_size, len(v_list), v_rows_of, w_places, quad),
        out_shape=out,
        in_specs=[VMEM] * (1 + len(v_list)) + [ANY if quad else VMEM] * len(w_list),
        out_specs=[VMEM] * len(out),
        scratch_shapes=scratch,
        cost_estimate=pl.CostEstimate(flops=1_000_000_000, bytes_accessed=8_000_000, transcendentals=0),
        name="project",
    )(mix, *v_list, *w_list)


def shards(n_group, n_prompt, queries, fresh_latent, latent_cache, selected, position, latent_gain, kv_up, out_weight):
    picks = queries.shape[2]
    width = out_weight.shape[1]
    rows_kv = kv_up.shape[0]
    rows_w = out_weight.shape[0]
    quad = n_group == 4 and n_prompt * rows_w == H * DV and n_prompt == 8
    m = DR // 2
    freqs = (10000.0 ** (-np.arange(m) / m)).astype(np.float32)
    freqs = jnp.asarray(np.tile(freqs, 4)[None, :])
    cache_t = jnp.swapaxes(latent_cache[0, 0], 0, 1)
    prepared = prep(
        n_group, quad, position, selected[0], fresh_latent[0, 0], cache_t, latent_gain[None, :], freqs, queries[0, 0]
    )
    blended = jnp.swapaxes(prepared[0], 0, 1)[None, None]
    pieces = cut(n_group, quad, kv_up, out_weight)
    both = ("group", "prompt")

    if not quad:
        _, keysel, q_out = prepared
        k_all, v_all = (lax.all_gather(t, "prompt", axis=0, tiled=True) for t in pieces)
        key_all = lax.all_gather(keysel, "group", axis=0)
        q_all = lax.all_to_all(q_out, "group", 0, 0)
        g = lax.axis_index("group")
        w_all = lax.all_gather(out_weight, "prompt", axis=0, tiled=True)
        w_own = w_all.reshape(H // n_group, n_group, DV, width)
        w_own = lax.dynamic_index_in_dim(w_own, g, 1, False).reshape(H // n_group * DV, width)
        whole = lambda: [(0, 0, LAT)]
        mix = attend(
            n_group, picks, position, [key_all[s] for s in range(n_group)], [q_all[s] for s in range(n_group)],
            [0] * n_group, [k_all], whole, lambda s: s,
        )
        (part,) = project(n_group, picks, mix, [v_all], whole, [w_own], None, False)
        got = lax.all_to_all(part, "group", 0, 0)
        attended = jnp.sum(got.astype(F32), 0).astype(BF16)
        return attended[None, None], blended

    _, far, near, far_q, own_q = prepared
    k_own, v_own, w_own = pieces
    ny = 2
    nz = n_prompt // ny
    over_x = [(g, g ^ 2) for g in range(n_group)]
    over_core = [(g, g ^ 1) for g in range(n_group)]
    over_y = [(p, p ^ 1) for p in range(n_prompt)]
    up_z = [(p, (p + ny) % n_prompt) for p in range(n_prompt)]
    holds = [(p, g) for p in range(n_prompt) for g in range(n_group) if p % ny == g % 2]
    w_up = [(g * n_prompt + p, g * n_prompt + (p + ny) % n_prompt) for p, g in holds]
    w_over = [(g * n_prompt + p, g * n_prompt + (p ^ 1)) for p, g in holds]

    far_in = lax.ppermute(far, "group", over_x)
    far_q_in = lax.ppermute(far_q, "group", over_x)
    near_in = lax.ppermute(near, "group", over_core)
    cross_in = lax.ppermute(far_in, "group", over_core)

    def spread(own):
        ring = [jnp.concatenate([own, lax.ppermute(own, "prompt", over_y)], 0)]
        for _ in range(nz - 1):
            ring.append(lax.ppermute(ring[-1], "prompt", up_z))
        return ring

    k_ring = spread(k_own)
    v_ring = spread(v_own)
    w_ring = [w_own]
    for _ in range(nz - 1):
        w_ring.append(lax.ppermute(w_ring[-1], both, w_up))
    w_side = [lax.ppermute(t, both, w_over) for t in w_ring]

    def ring_rows():
        p = lax.axis_index("prompt")
        y = p % ny
        out = []
        for k in range(nz):
            layer = lax.rem(p // ny + nz - k, nz)
            out.append(((layer * ny + y) * rows_kv, 0, rows_kv))
            out.append(((layer * ny + 1 - y) * rows_kv, rows_kv, rows_kv))
        return out

    def w_places():
        p = lax.axis_index("prompt")
        g = lax.axis_index("group")
        return p % ny == g % 2, [lax.rem(p // ny + nz - k, nz) * DV for k in range(nz)]

    slot_group = lambda s: lax.axis_index("group") ^ s
    q_at = ROW + SELROWS
    mix = attend(
        n_group, picks, position, [far, near_in, far_in, cross_in], [own_q, near_in, far_q_in, cross_in],
        [0, q_at, 0, q_at], [t for t in k_ring for _ in range(ny)], ring_rows, slot_group,
    )
    send, keep = project(
        n_group, picks, mix, [t for t in v_ring for _ in range(ny)], ring_rows, w_ring + w_side, w_places, True
    )
    sums = keep + lax.ppermute(send, "group", over_core).astype(F32)
    last = lax.ppermute(sums[1].astype(BF16), "group", over_x)
    attended = (sums[0] + last.astype(F32)).astype(BF16)
    return attended[None, None], blended


def solution(mesh):
    in_specs = (
        P("prompt", "group", None, None),
        P("prompt", "group", None, None),
        P("prompt", "group", None, None),
        P("prompt", "group", None),
        P("prompt", None),
        P(),
        P("prompt", None),
        P("prompt", None),
    )
    out_specs = (P("prompt", "group", None, None), P("prompt", "group", None, None))
    body = functools.partial(shards, mesh.shape["group"], mesh.shape["prompt"])
    return jax.shard_map(body, mesh=mesh, in_specs=in_specs, out_specs=out_specs, check_vma=False)
```

```python
import functools

import jax
import jax.numpy as jnp
import numpy as np
from jax import lax
from jax.experimental import pallas as pl
from jax.experimental.pallas import tpu as pltpu
from jax.sharding import PartitionSpec as P


H = 16
DN = 128
DR = 64
DV = 128
LAT = 512
ROW = LAT + DR
SELROWS = 16
LOW = 256
NEG = -1e30
F32 = jnp.float32
BF16 = jnp.bfloat16


VMEM = pl.BlockSpec(memory_space=pltpu.VMEM)
SMEM = pl.BlockSpec(memory_space=pltpu.SMEM)
ANY = pl.BlockSpec(memory_space=pl.ANY)


def iota(shape, axis):
    return lax.broadcasted_iota(jnp.int32, shape, axis)


def column_of(row):
    n = row.shape[-1]
    square = jnp.where(iota((n, n), 0) == iota((n, n), 1), jnp.broadcast_to(row, (n, n)), 0.0)
    return jnp.sum(square, -1, keepdims=True)


def rotate(tile, cosine, sine):
    lane = iota(tile.shape, 1) % DR
    other = jnp.where(lane < DR // 2, pltpu.roll(tile, 2 * DR - DR // 2, 1), pltpu.roll(tile, DR // 2, 1))
    return tile * cosine + other * sine


def prep_kernel(group_size, quad, position, selected, fresh, cache, gain, freqs, queries, *refs):
    g = lax.axis_index("group")
    per = H // group_size
    picks = fresh.shape[0]
    length = cache.shape[1]
    if quad:
        blended, far, near, own_q, q_all = refs
    else:
        blended, far, out_q, q_all = refs
    sel_row = selected[...].astype(F32)
    sel = column_of(sel_row)
    place = position[0, g].astype(F32) * length + sel
    angle = place * freqs[...]
    cosine = jnp.cos(angle)
    sine = jnp.sin(angle)
    sine = jnp.where(iota(sine.shape, 1) % DR < DR // 2, -sine, sine)

    for pair in range(H // 2):
        base = pair * 2 * (DN + DR)
        tile1 = queries[:, base + 128 : base + 256].astype(F32)
        tile2 = queries[:, base + 256 : base + 384].astype(F32)
        low = iota(tile1.shape, 1) < DR
        turned = rotate(jnp.where(low, tile1, tile2), cosine, sine)
        other = pltpu.roll(turned, DR, 1)
        second = pltpu.roll(jnp.where(low, tile2, tile1), DR, 1)
        for odd in range(2):
            head = 2 * pair + odd
            slot, r = divmod(head, group_size)
            nope = second.astype(BF16) if odd else queries[:, base : base + 128]
            q_all[r, 0:picks, slot * DN : (slot + 1) * DN] = nope
            want_high = slot % 2 == 1
            piece = (turned if (odd == 1) == want_high else other).astype(BF16)
            col = slot // 2 * 128 + (DR if want_high else 0)
            mine = piece[:, DR:] if want_high else piece[:, :DR]
            half = picks // 2
            q_all[r, picks : picks + half, col : col + DR] = mine[:half]
            q_all[r, picks : picks + half, per * DR + col : per * DR + col + DR] = mine[half:]

    latent = fresh[:, :LAT].astype(F32)
    factor = lax.rsqrt(jnp.mean(latent * latent, -1, keepdims=True) + 1e-06)
    normed = (latent * factor * gain[...].astype(F32)).astype(BF16)
    tail = fresh[:, LAT:].astype(F32)
    swapped = jnp.concatenate([tail[:, DR // 2 :], tail[:, : DR // 2]], 1)
    turned = (tail * cosine[:, :DR] + swapped * sine[:, :DR]).astype(BF16)
    hot = iota((picks, length), 1).astype(F32) == sel
    hot_bf = hot.astype(BF16)
    hit = jnp.sum(hot.astype(F32), 0, keepdims=True) > 0.5
    over_rows = (((0,), (0,)), ((), ()))
    for start, rows in ((0, normed), (LAT, turned)):
        placed = lax.dot_general(rows, hot_bf, over_rows, preferred_element_type=F32)
        stop = start + rows.shape[1]
        mixed = jnp.where(hit, placed, cache[start:stop, :].astype(F32)).astype(BF16)
        blended[start:stop, :] = mixed
        far[start:stop, :] = mixed
        if quad:
            near[start:stop, :] = mixed
    high = jnp.floor(sel_row / LOW)
    low = sel_row - high * LOW
    at = iota((SELROWS, picks), 0)
    coded = jnp.where(at == 0, low, jnp.where(at == 1, high, 0.0)).astype(BF16)
    coded = jnp.concatenate([coded, jnp.zeros((SELROWS, length - picks), BF16)], 1)
    far[ROW : ROW + SELROWS, :] = coded
    if quad:
        near[ROW : ROW + SELROWS, :] = coded
        x, c = g // 2, g % 2
        rows = q_all.shape[1]
        far[ROW + SELROWS : ROW + SELROWS + rows, :] = q_all[2 * (1 - c) + 1 - x]
        far[ROW + SELROWS + rows :, :] = q_all[2 * c + 1 - x]
        near[ROW + SELROWS :, :] = q_all[2 * (1 - c) + x]
        own_q[...] = q_all[2 * c + x]
    else:
        out_q[...] = q_all[...]


def prep(group_size, quad, position, selected, fresh, cache, gain, freqs, queries):
    picks = fresh.shape[0]
    length = cache.shape[1]
    per = H // group_size
    q_rows = picks + picks // 2
    width = per * DN
    keys = ROW + SELROWS
    out = [jax.ShapeDtypeStruct((ROW, length), BF16)]
    if quad:
        out += [jax.ShapeDtypeStruct((keys + n * q_rows, length), BF16) for n in (2, 1)]
        out += [jax.ShapeDtypeStruct((q_rows, width), BF16)]
    else:
        out += [jax.ShapeDtypeStruct((keys, length), BF16), jax.ShapeDtypeStruct((group_size, q_rows, width), BF16)]
    return pl.pallas_call(
        functools.partial(prep_kernel, group_size, quad),
        out_shape=out,
        in_specs=[SMEM] + [VMEM] * 6,
        out_specs=[VMEM] * len(out),
        scratch_shapes=[pltpu.VMEM((group_size, q_rows, width), BF16)],
        cost_estimate=pl.CostEstimate(flops=50_000_000, bytes_accessed=4_000_000, transcendentals=0),
        name="prep",
    )(position, selected, fresh, cache, gain, freqs, queries)


def cut_kernel(group_size, quad, kv, w, kv_out, *refs):
    g = lax.axis_index("group")
    per = H // group_size
    rows = kv.shape[0]
    x, c = g // 2, g % 2
    r = 2 * c + x if quad else g
    sems = refs[-1]
    copies = []
    if quad:
        half = DV // 2
        take = w.at[pl.ds(pl.multiple_of(x * DV + c * half, half), half), :]
        copies.append(pltpu.make_async_copy(take, refs[0], sems.at[2 * per]))
    for slot in range(per):
        at = (slot * group_size + r) * (DN + DV)
        for k in range(2):
            copies.append(
                pltpu.make_async_copy(
                    kv.at[:, pl.ds(pl.multiple_of(at + k * DN, DN), DN)],
                    kv_out.at[k * rows : (k + 1) * rows, slot * DN : (slot + 1) * DN],
                    sems.at[2 * slot + k],
                )
            )
    for copy in copies:
        copy.start()
    for copy in copies:
        copy.wait()


def cut(group_size, quad, kv, w):
    rows = kv.shape[0]
    per = H // group_size
    out = [jax.ShapeDtypeStruct((2 * rows, per * DN), BF16)]
    if quad:
        out += [jax.ShapeDtypeStruct((DV // 2, w.shape[1]), BF16)]
    return pl.pallas_call(
        functools.partial(cut_kernel, group_size, quad),
        out_shape=out,
        in_specs=[ANY] * 2,
        out_specs=[VMEM] * len(out),
        scratch_shapes=[pltpu.SemaphoreType.DMA((2 * per + 1,))],
        cost_estimate=pl.CostEstimate(flops=1_000_000, bytes_accessed=2_000_000, transcendentals=0),
        name="cut",
    )(kv, w)


def attend_kernel(group_size, quad, key_at, q_at, kv_places, slot_group, picks, position, *refs):
    n = group_size
    n_in = n + len([i for i, _ in q_at if i >= n]) + len(kv_places()[0])
    ins, outs = refs[:n_in], refs[n_in : -11]
    keys, coded, q_in, k_up, v_up, query, acc, peak, total, mix, sems = refs[-11:]
    slots = group_size
    per = H // group_size
    length = keys.shape[2]
    rows = per * picks
    half = picks // 2
    last = (((1,), (1,)), ((), ()))

    kv_refs = ins[n_in - len(kv_places()[0]) :]
    early, late = [], []
    firsts, count = kv_places()
    for i, (ref, first) in enumerate(zip(kv_refs, firsts)):
        at = pl.multiple_of(first, count)
        early.append(pltpu.make_async_copy(ref.at[0:count, :], k_up.at[pl.ds(at, count), :], sems.at[0, i]))
        late.append(pltpu.make_async_copy(ref.at[count : 2 * count, :], v_up.at[pl.ds(at, count), :], sems.at[1, i]))
    moves = []
    for s in range(slots):
        i, start = q_at[s]
        early.append(pltpu.make_async_copy(ins[i].at[start : start + picks + half, :], q_in.at[s], sems.at[2, s]))
        moves.append(pltpu.make_async_copy(ins[key_at[s]].at[ROW : ROW + SELROWS, :], coded.at[s], sems.at[3, s]))
        moves.append(pltpu.make_async_copy(ins[key_at[s]].at[0:ROW, :], keys.at[s], sems.at[4, s]))
    for copy in early + moves + late:
        copy.start()
    for copy in early:
        copy.wait()
    for s in range(slots):
        for j in range(per):
            folded = q_in[s, picks:, :]
            for k in range(2):
                at = k * per * DR + j * DR
                query[s, j * picks + k * half : j * picks + (k + 1) * half, LAT:] = folded[:, at : at + DR]
    for j in range(per):
        plain = jnp.concatenate([q_in[s, 0:picks, j * DN : (j + 1) * DN] for s in range(slots)], 0)
        absorbed = lax.dot_general(plain, k_up[:, j * DN : (j + 1) * DN], last, preferred_element_type=F32)
        absorbed = absorbed.astype(BF16)
        for s in range(slots):
            query[s, j * picks : (j + 1) * picks, :LAT] = absorbed[s * picks : (s + 1) * picks]
    for copy in moves:
        copy.wait()

    scale = (DN + DR) ** (-0.5) * float(np.log2(np.e))

    def one(a, _):
        place = position[0, slot_group(a)]
        code = coded[a][:, 0:picks].astype(F32)
        sel = column_of(code[0:1] + LOW * code[1:2])
        sel = jnp.concatenate([sel] * per, 0)
        s = jnp.dot(query[a], keys[a], preferred_element_type=F32) * scale
        allowed = iota((rows, length), 1).astype(F32) <= sel
        s = jnp.where(allowed, s, NEG)
        top = jnp.max(s, -1, keepdims=True)
        p = jnp.exp2(s - top)
        peak[...] = top
        total[...] = jnp.sum(p, -1, keepdims=True)
        acc[...] = lax.dot_general(p.astype(BF16), keys[a, :LAT, :], last, preferred_element_type=F32)

        def other(b, _):
            @pl.when(position[0, slot_group(b)] < place)
            def _():
                s = jnp.dot(query[a], keys[b], preferred_element_type=F32) * scale
                old = peak[...]
                top = jnp.maximum(old, jnp.max(s, -1, keepdims=True))
                decay = jnp.exp2(old - top)
                p = jnp.exp2(s - top)
                peak[...] = top
                total[...] = total[...] * decay + jnp.sum(p, -1, keepdims=True)
                acc[...] = acc[...] * decay + lax.dot_general(
                    p.astype(BF16), keys[b, :LAT, :], last, preferred_element_type=F32
                )

            return 0

        lax.fori_loop(0, slots, other, 0)
        done = (acc[...] / total[...]).astype(BF16)
        for j in range(per):
            mix[j, pl.ds(pl.multiple_of(a * picks, picks), picks), :] = done[j * picks : (j + 1) * picks]
        return 0

    lax.fori_loop(0, slots, one, 0)
    for copy in late:
        copy.wait()
    for j in range(per):
        up = jnp.dot(mix[j], v_up[:, j * DV : (j + 1) * DV], preferred_element_type=F32)
        if quad:
            keep, send = outs
            c = lax.axis_index("group") % 2
            width = DV // 2
            low, high = up[:, :width], up[:, width:]
            keep[:, j * width : (j + 1) * width] = jnp.where(c == 0, low, high).astype(BF16)
            send[:, j * width : (j + 1) * width] = jnp.where(c == 0, high, low).astype(BF16)
        else:
            outs[0][:, j * DV : (j + 1) * DV] = up.astype(BF16)


def attend(group_size, quad, picks, position, ins, key_at, q_at, kv_places, slot_group):
    per = H // group_size
    length = ins[0].shape[1]
    rows = per * picks
    slots = group_size
    n_kv = len(kv_places()[0])
    kernel = functools.partial(attend_kernel, group_size, quad, key_at, q_at, kv_places, slot_group, picks)
    tokens = slots * picks
    if quad:
        out = [jax.ShapeDtypeStruct((tokens, per * DV // 2), BF16)] * 2
    else:
        out = [jax.ShapeDtypeStruct((tokens, per * DV), BF16)]
    return pl.pallas_call(
        kernel,
        out_shape=out,
        in_specs=[SMEM] + [ANY] * len(ins),
        out_specs=[VMEM] * len(out),
        scratch_shapes=[
            pltpu.VMEM((slots, ROW, length), BF16),
            pltpu.VMEM((slots, SELROWS, length), BF16),
            pltpu.VMEM((slots, picks + picks // 2, per * DN), BF16),
            pltpu.VMEM((LAT, per * DN), BF16),
            pltpu.VMEM((LAT, per * DV), BF16),
            pltpu.VMEM((slots, rows, ROW), BF16),
            pltpu.VMEM((rows, LAT), F32),
            pltpu.VMEM((rows, 1), F32),
            pltpu.VMEM((rows, 1), F32),
            pltpu.VMEM((per, tokens, LAT), BF16),
            pltpu.SemaphoreType.DMA((5, max(slots, n_kv))),
        ],
        cost_estimate=pl.CostEstimate(flops=5_000_000_000, bytes_accessed=8_000_000, transcendentals=0),
        name="attend",
    )(position, *ins)


def project_kernel(group_size, quad, w_places, *refs):
    if quad:
        keep_in, recv_in = refs[:2]
        w_refs = refs[2:-5]
        send, keep, heads, w, sems = refs[-5:]
        firsts, count = w_places()
        copies = []
        for i, (ref, first) in enumerate(zip(w_refs, firsts)):
            target = w.at[pl.ds(pl.multiple_of(first, count), count), :]
            copies.append(pltpu.make_async_copy(ref, target, sems.at[i]))
        for copy in copies:
            copy.start()
        part = keep_in.shape[1]
        heads[:, :part] = keep_in[...]
        rows = send.shape[1]
        for s in range(group_size):
            heads[s * rows : (s + 1) * rows, part:] = recv_in[(s ^ 1) * rows : ((s ^ 1) + 1) * rows]
        for copy in copies:
            copy.wait()
    else:
        heads, w, send = refs
    width = w.shape[1]
    step = min(width, 512)
    picks = send.shape[1]
    for at in range(0, width, step):
        out = jnp.dot(heads[...], w[:, at : at + step], preferred_element_type=F32)
        for s in range(group_size):
            piece = out[s * picks : (s + 1) * picks]
            if not quad:
                send[s, :, at : at + step] = piece.astype(BF16)
            elif s % 2:
                send[s // 2, :, at : at + step] = piece.astype(BF16)
            else:
                keep[s // 2, :, at : at + step] = piece


def project(group_size, quad, picks, heads, w_list, w_places):
    width = w_list[0].shape[1]
    scratch = []
    if quad:
        part = heads[0].shape[1]
        out = [jax.ShapeDtypeStruct((2, picks, width), BF16), jax.ShapeDtypeStruct((2, picks, width), F32)]
        scratch = [
            pltpu.VMEM((group_size * picks, 2 * part), BF16),
            pltpu.VMEM((2 * part, width), BF16),
            pltpu.SemaphoreType.DMA((len(w_list),)),
        ]
    else:
        out = [jax.ShapeDtypeStruct((group_size, picks, width), BF16)]
    return pl.pallas_call(
        functools.partial(project_kernel, group_size, quad, w_places),
        out_shape=out,
        in_specs=[VMEM] * len(heads) + [ANY if quad else VMEM] * len(w_list),
        out_specs=[VMEM] * len(out),
        scratch_shapes=scratch,
        cost_estimate=pl.CostEstimate(flops=1_000_000_000, bytes_accessed=8_000_000, transcendentals=0),
        name="project",
    )(*heads, *w_list)


def layer(n_group, n_prompt, queries, fresh_latent, latent_cache, selected, position, latent_gain, kv_up, out_weight):
    picks = queries.shape[2]
    width = out_weight.shape[1]
    rows_kv = kv_up.shape[0]
    per = H // n_group
    quad = n_group == 4 and n_prompt == 8 and out_weight.shape[0] == 2 * DV
    m = DR // 2
    freqs = (10000.0 ** (-np.arange(m) / m)).astype(np.float32)
    freqs = jnp.asarray(np.tile(freqs, 4)[None, :])
    cache_t = jnp.swapaxes(latent_cache[0, 0], 0, 1)
    pieces = cut(n_group, quad, kv_up, out_weight)
    prepared = prep(
        n_group, quad, position, selected[0], fresh_latent[0, 0], cache_t, latent_gain[None, :], freqs,
        queries[0, 0],
    )
    blended = jnp.swapaxes(prepared[0], 0, 1)[None, None]

    if not quad:
        _, keysel, q_out = prepared
        kv_all = lax.all_gather(pieces[0], "prompt", axis=0)
        key_all = lax.all_gather(keysel, "group", axis=0)
        q_all = lax.all_to_all(q_out, "group", 0, 0)
        g = lax.axis_index("group")
        w_all = lax.all_gather(out_weight, "prompt", axis=0, tiled=True)
        w_own = lax.dynamic_index_in_dim(w_all.reshape(per, n_group, DV, width), g, 1, False)
        ins = [key_all[s] for s in range(n_group)] + [q_all[s] for s in range(n_group)]
        places = lambda: ([p * rows_kv for p in range(n_prompt)], rows_kv)
        heads = attend(
            n_group, quad, picks, position, ins + [kv_all[p] for p in range(n_prompt)], list(range(n_group)),
            [(n_group + s, 0) for s in range(n_group)], places, lambda s: s,
        )
        (part,) = project(n_group, quad, picks, heads, [w_own.reshape(per * DV, width)], None)
        got = lax.all_to_all(part, "group", 0, 0)
        attended = jnp.sum(got.astype(F32), 0).astype(BF16)
        return attended[None, None], blended

    _, far, near, own_q = prepared
    kv_own, w_own = pieces
    ny = 2
    nz = n_prompt // ny
    over_x = [(g, g ^ 2) for g in range(n_group)]
    over_core = [(g, g ^ 1) for g in range(n_group)]
    over_y = [(p, p ^ 1) for p in range(n_prompt)]
    up_z = lambda d: [(p, (p + d * ny) % n_prompt) for p in range(n_prompt)]

    def spread(own):
        column = [own] + [lax.ppermute(own, "prompt", up_z(k)) for k in range(1, nz)]
        return column + [lax.ppermute(t, "prompt", over_y) for t in column]

    kv = spread(kv_own)
    w = spread(w_own)
    far_in = lax.ppermute(far, "group", over_x)
    near_in = lax.ppermute(near, "group", over_core)
    cross_in = lax.ppermute(far_in, "group", over_core)

    def layers():
        z = lax.axis_index("prompt") // ny
        return [lax.rem(z + nz - k, nz) for k in range(nz)]

    def kv_places():
        y = lax.axis_index("prompt") % ny
        return [(z * ny + at) * rows_kv for at in (y, 1 - y) for z in layers()], rows_kv

    def w_places():
        y = lax.axis_index("prompt") % ny
        other = lax.rem(y + lax.axis_index("group"), 2)
        count = DV // 2
        return [(at * nz + z) * count for at in (other, 1 - other) for z in layers()], count

    slot_group = lambda s: lax.axis_index("group") ^ s
    q_rows = picks + picks // 2
    q_start = ROW + SELROWS
    keep, send = attend(
        n_group, quad, picks, position, [far, near_in, far_in, cross_in, own_q] + kv, [0, 1, 2, 3],
        [(4, 0), (1, q_start), (2, q_start + q_rows), (3, q_start)], kv_places, slot_group,
    )
    got = lax.ppermute(send, "group", over_core)
    send, keep = project(n_group, quad, picks, [keep, got], w, w_places)
    sums = keep + lax.ppermute(send, "group", over_core).astype(F32)
    last = lax.ppermute(sums[1].astype(BF16), "group", over_x)
    attended = (sums[0] + last.astype(F32)).astype(BF16)
    return attended[None, None], blended


def solution(mesh):
    in_specs = (
        P("prompt", "group", None, None),
        P("prompt", "group", None, None),
        P("prompt", "group", None, None),
        P("prompt", "group", None),
        P("prompt", None),
        P(),
        P("prompt", None),
        P("prompt", None),
    )
    out_specs = (P("prompt", "group", None, None), P("prompt", "group", None, None))
    body = functools.partial(layer, mesh.shape["group"], mesh.shape["prompt"])
    return jax.shard_map(body, mesh=mesh, in_specs=in_specs, out_specs=out_specs, check_vma=False)
```

```python
import functools

import jax
import jax.numpy as jnp
import numpy as np
from jax import lax
from jax.experimental import pallas as pl
from jax.experimental.pallas import tpu as pltpu
from jax.sharding import PartitionSpec as P


H = 16
DN = 128
DR = 64
DV = 128
LAT = 512
ROW = LAT + DR
SELROWS = 16
LOW = 256
NEG = -1e30
F32 = jnp.float32
BF16 = jnp.bfloat16


VMEM = pl.BlockSpec(memory_space=pltpu.VMEM)
SMEM = pl.BlockSpec(memory_space=pltpu.SMEM)
HBM = pl.BlockSpec(memory_space=pltpu.HBM)


def iota(shape, axis):
    return lax.broadcasted_iota(jnp.int32, shape, axis)


def column_of(row):
    n = row.shape[-1]
    square = jnp.where(iota((n, n), 0) == iota((n, n), 1), jnp.broadcast_to(row, (n, n)), 0.0)
    return jnp.sum(square, -1, keepdims=True)


def rotate(tile, cosine, sine):
    lane = iota(tile.shape, 1) % DR
    other = jnp.where(lane < DR // 2, pltpu.roll(tile, 2 * DR - DR // 2, 1), pltpu.roll(tile, DR // 2, 1))
    return tile * cosine + other * sine


def prep_kernel(group_size, quad, position, selected, gain, freqs, fresh, cache, queries, *refs):
    g = lax.axis_index("group")
    per = H // group_size
    picks = fresh.shape[0]
    length = cache.shape[1]
    if quad:
        blended, far, near, own_q, q_all = refs
    else:
        blended, far, out_q, q_all = refs
    sel_row = selected[...].astype(F32)
    sel = column_of(sel_row)
    place = position[0, g].astype(F32) * length + sel
    angle = place * freqs[...]
    cosine = jnp.cos(angle)
    sine = jnp.sin(angle)
    sine = jnp.where(iota(sine.shape, 1) % DR < DR // 2, -sine, sine)

    for pair in range(H // 2):
        base = pair * 2 * (DN + DR)
        tile1 = queries[:, base + 128 : base + 256].astype(F32)
        tile2 = queries[:, base + 256 : base + 384].astype(F32)
        low = iota(tile1.shape, 1) < DR
        turned = rotate(jnp.where(low, tile1, tile2), cosine, sine)
        other = pltpu.roll(turned, DR, 1)
        second = pltpu.roll(jnp.where(low, tile2, tile1), DR, 1)
        for odd in range(2):
            head = 2 * pair + odd
            slot, r = divmod(head, group_size)
            nope = second.astype(BF16) if odd else queries[:, base : base + 128]
            q_all[r, 0:picks, slot * DN : (slot + 1) * DN] = nope
            want_high = slot % 2 == 1
            piece = (turned if (odd == 1) == want_high else other).astype(BF16)
            col = slot // 2 * 128 + (DR if want_high else 0)
            mine = piece[:, DR:] if want_high else piece[:, :DR]
            half = picks // 2
            q_all[r, picks : picks + half, col : col + DR] = mine[:half]
            q_all[r, picks : picks + half, per * DR + col : per * DR + col + DR] = mine[half:]

    latent = fresh[:, :LAT].astype(F32)
    factor = lax.rsqrt(jnp.mean(latent * latent, -1, keepdims=True) + 1e-06)
    normed = (latent * factor * gain[...].astype(F32)[None, :]).astype(BF16)
    tail = fresh[:, LAT:].astype(F32)
    swapped = jnp.concatenate([tail[:, DR // 2 :], tail[:, : DR // 2]], 1)
    turned = (tail * cosine[:, :DR] + swapped * sine[:, :DR]).astype(BF16)
    hot = iota((picks, length), 1).astype(F32) == sel
    hot_bf = hot.astype(BF16)
    hit = jnp.sum(hot.astype(F32), 0, keepdims=True) > 0.5
    over_rows = (((0,), (0,)), ((), ()))
    for start, rows in ((0, normed), (LAT, turned)):
        placed = lax.dot_general(rows, hot_bf, over_rows, preferred_element_type=F32)
        stop = start + rows.shape[1]
        mixed = jnp.where(hit, placed, cache[start:stop, :].astype(F32)).astype(BF16)
        blended[start:stop, :] = mixed
        far[start:stop, :] = mixed
        if quad:
            near[start:stop, :] = mixed
    high = jnp.floor(sel_row / LOW)
    low = sel_row - high * LOW
    at = iota((SELROWS, picks), 0)
    coded = jnp.where(at == 0, low, jnp.where(at == 1, high, 0.0)).astype(BF16)
    coded = jnp.concatenate([coded, jnp.zeros((SELROWS, length - picks), BF16)], 1)
    far[ROW : ROW + SELROWS, :] = coded
    if quad:
        near[ROW : ROW + SELROWS, :] = coded
        x, c = g // 2, g % 2
        rows = q_all.shape[1]
        far[ROW + SELROWS : ROW + SELROWS + rows, :] = q_all[2 * (1 - c) + 1 - x]
        far[ROW + SELROWS + rows :, :] = q_all[2 * c + 1 - x]
        near[ROW + SELROWS :, :] = q_all[2 * (1 - c) + x]
        own_q[...] = q_all[2 * c + x]
    else:
        out_q[...] = q_all[...]


def prep(group_size, quad, position, selected, gain, freqs, fresh, cache, queries):
    picks = fresh.shape[0]
    length = cache.shape[1]
    per = H // group_size
    q_rows = picks + picks // 2
    width = per * DN
    keys = ROW + SELROWS
    out = [jax.ShapeDtypeStruct((ROW, length), BF16)]
    if quad:
        out += [jax.ShapeDtypeStruct((keys + n * q_rows, length), BF16) for n in (2, 1)]
        out += [jax.ShapeDtypeStruct((q_rows, width), BF16)]
    else:
        out += [jax.ShapeDtypeStruct((keys, length), BF16), jax.ShapeDtypeStruct((group_size, q_rows, width), BF16)]
    return pl.pallas_call(
        functools.partial(prep_kernel, group_size, quad),
        out_shape=out,
        in_specs=[SMEM] + [VMEM] * 6,
        out_specs=[VMEM] * len(out),
        scratch_shapes=[pltpu.VMEM((group_size, q_rows, width), BF16)],
        cost_estimate=pl.CostEstimate(flops=50_000_000, bytes_accessed=4_000_000, transcendentals=0),
        compiler_params=pltpu.CompilerParams(vmem_limit_bytes=16 << 20),
        name="prep",
    )(
        position,
        *[pltpu.with_memory_space_constraint(t, pltpu.HBM) for t in (selected, gain, freqs)],
        *[near_core(t) for t in (fresh, cache, queries)],
    )


def cut_kernel(group_size, quad, n_staged, kv, w, *refs):
    staged, kv_out, refs = refs[:n_staged], refs[n_staged], refs[n_staged + 1 :]
    g = lax.axis_index("group")
    per = H // group_size
    rows = kv.shape[0]
    x, c = g // 2, g % 2
    r = 2 * c + x if quad else g
    sems = refs[-1]
    copies = []
    for i, source in enumerate(staged):
        copies.append(pltpu.make_async_copy(source, refs[i - n_staged - 1], sems.at[2 * per + 1 + i]))
    if quad:
        half = DV // 2
        take = w.at[pl.ds(pl.multiple_of(x * DV + c * half, half), half), :]
        copies.append(pltpu.make_async_copy(take, refs[0], sems.at[2 * per]))
    for slot in range(per):
        at = (slot * group_size + r) * (DN + DV)
        for k in range(2):
            copies.append(
                pltpu.make_async_copy(
                    kv.at[:, pl.ds(pl.multiple_of(at + k * DN, DN), DN)],
                    kv_out.at[k * rows : (k + 1) * rows, slot * DN : (slot + 1) * DN],
                    sems.at[2 * slot + k],
                )
            )
    for copy in copies:
        copy.start()
    for copy in copies:
        copy.wait()


def cut(group_size, quad, kv, w, staged):
    rows = kv.shape[0]
    per = H // group_size
    out = [jax.ShapeDtypeStruct((2 * rows, per * DN), BF16)]
    if quad:
        out += [jax.ShapeDtypeStruct((DV // 2, w.shape[1]), BF16)]
    out += [pltpu.VMEM(t.shape, t.dtype) for t in staged]
    n = len(staged)
    made = pl.pallas_call(
        functools.partial(cut_kernel, group_size, quad, n),
        out_shape=out,
        in_specs=[HBM] * (2 + n),
        out_specs=[VMEM] * len(out),
        scratch_shapes=[pltpu.SemaphoreType.DMA((2 * per + 1 + n,))],
        cost_estimate=pl.CostEstimate(flops=1_000_000, bytes_accessed=2_000_000, transcendentals=0),
        compiler_params=pltpu.CompilerParams(vmem_limit_bytes=8 << 20),
        name="cut",
    )(*[pltpu.with_memory_space_constraint(t, pltpu.HBM) for t in (kv, w, *staged)])
    return made[:-n], made[-n:]


def near_core(x):
    return pltpu.with_memory_space_constraint(x, pltpu.VMEM)


def absorb_kernel(group_size, key_at, q_at, kv_places, picks, *refs):
    n = group_size
    n_in = n + len([i for i, _ in q_at if i >= n]) + len(kv_places()[0])
    ins = refs[:n_in]
    keys, turned_keys, coded, query, v_up, k_up, plain, rope = refs[n_in:]
    slots = group_size
    per = H // group_size
    half = picks // 2
    last = (((1,), (1,)), ((), ()))
    kv_refs = ins[n_in - len(kv_places()[0]) :]
    firsts, count = kv_places()
    for ref, at in zip(kv_refs, firsts):
        at = pl.ds(pl.multiple_of(at, count), count)
        k_up[at, :] = ref[0:count, :]
        v_up[at, :] = ref[count : 2 * count, :]
    plain[...] = jnp.zeros_like(plain)
    for s in range(slots):
        keys[s] = ins[key_at[s]][0:ROW, :]
        turned_keys[s] = jnp.swapaxes(ins[key_at[s]][0:ROW, :], 0, 1)
        coded[s] = ins[key_at[s]][ROW : ROW + SELROWS, :]
        i, start = q_at[s]
        folded = ins[i][start + picks : start + picks + half, :]
        for j in range(per):
            own = slice(j * DN, (j + 1) * DN)
            plain[s, j * picks : (j + 1) * picks, own] = ins[i][start : start + picks, own]
            for k in range(2):
                at = k * per * DR + j * DR
                rope[s, j * picks + k * half : j * picks + (k + 1) * half, :] = folded[:, at : at + DR]
    eye = (iota((DR, DR), 0) == iota((DR, DR), 1)).astype(BF16)
    for s in range(slots):
        absorbed = lax.dot_general(k_up[...], plain[s], last, preferred_element_type=F32)
        query[s, :LAT, :] = absorbed.astype(BF16)
        query[s, LAT:, :] = lax.dot_general(eye, rope[s], last, preferred_element_type=F32).astype(BF16)


def absorb(group_size, picks, ins, key_at, q_at, kv_places):
    per = H // group_size
    length = ins[0].shape[1]
    rows = per * picks
    slots = group_size
    shapes = [
        (slots, ROW, length), (slots, length, ROW), (slots, SELROWS, length), (slots, ROW, rows), (LAT, per * DV)
    ]
    return pl.pallas_call(
        functools.partial(absorb_kernel, group_size, key_at, q_at, kv_places, picks),
        out_shape=[jax.ShapeDtypeStruct(shape, BF16) for shape in shapes],
        in_specs=[VMEM] * len(ins),
        out_specs=[VMEM] * len(shapes),
        scratch_shapes=[
            pltpu.VMEM((LAT, per * DN), BF16),
            pltpu.VMEM((slots, rows, per * DN), BF16),
            pltpu.VMEM((slots, rows, DR), BF16),
        ],
        cost_estimate=pl.CostEstimate(flops=1_000_000_000, bytes_accessed=8_000_000, transcendentals=0),
        compiler_params=pltpu.CompilerParams(vmem_limit_bytes=24 << 20),
        name="absorb",
    )(*[near_core(t) for t in ins])


def attend_kernel(group_size, quad, places, slot_group, picks, n_out, position, *refs):
    keys, turned_keys, coded, query, v_up = refs[:5]
    outs = refs[-n_out:]
    slots = group_size
    per = H // group_size
    length = keys.shape[2]
    rows = per * picks
    first = (((0,), (0,)), ((), ()))
    at_place = []
    for place in range(slots):
        found = 0
        for s in range(1, slots):
            found = jnp.where(position[0, slot_group(s)] == place, s, found)
        at_place.append(found)
    scale = (DN + DR) ** (-0.5) * float(np.log2(np.e))
    for o in places:
        a = at_place[o]
        q = query[a]
        code = coded[a][:, 0:picks].astype(F32)
        sel = code[0:1] + LOW * code[1:2]
        sel = jnp.concatenate([sel] * per, 1)
        scores = [jnp.dot(turned_keys[at_place[k]], q, preferred_element_type=F32) * scale for k in range(o + 1)]
        allowed = iota((length, rows), 0).astype(F32) <= sel
        scores[o] = jnp.where(allowed, scores[o], NEG)
        top = functools.reduce(jnp.maximum, [jnp.max(s, 0, keepdims=True) for s in scores])
        probs = [jnp.exp2(s - top) for s in scores]
        total = functools.reduce(jnp.add, [jnp.sum(p, 0, keepdims=True) for p in probs])
        mixed = functools.reduce(
            jnp.add,
            [
                jnp.dot(keys[at_place[k], :LAT, :], probs[k].astype(BF16), preferred_element_type=F32)
                for k in range(o + 1)
            ],
        )
        mixed = (mixed * (1.0 / total)).astype(BF16)
        up = lax.dot_general(mixed, v_up[...], first, preferred_element_type=F32)
        at = pl.ds(pl.multiple_of(a * picks, picks), picks)
        for j in range(per):
            head = up[j * picks : (j + 1) * picks, j * DV : (j + 1) * DV]
            if quad:
                keep, send = outs
                c = lax.axis_index("group") % 2
                width = DV // 2
                low, high = head[:, :width], head[:, width:]
                keep[at, j * width : (j + 1) * width] = jnp.where(c == 0, low, high).astype(BF16)
                send[at, j * width : (j + 1) * width] = jnp.where(c == 0, high, low).astype(BF16)
            else:
                outs[0][at, j * DV : (j + 1) * DV] = head.astype(BF16)


def attend(group_size, quad, picks, position, ready, places, slot_group, before):
    per = H // group_size
    tokens = group_size * picks
    if quad:
        out = [jax.ShapeDtypeStruct((tokens, per * DV // 2), BF16)] * 2
    else:
        out = [jax.ShapeDtypeStruct((tokens, per * DV), BF16)]
    return pl.pallas_call(
        functools.partial(attend_kernel, group_size, quad, places, slot_group, picks, len(out)),
        out_shape=out,
        in_specs=[SMEM] + [VMEM] * (len(ready) + len(before)),
        out_specs=[VMEM] * len(out),
        input_output_aliases={1 + len(ready) + i: i for i in range(len(before))},
        cost_estimate=pl.CostEstimate(flops=3_000_000_000, bytes_accessed=8_000_000, transcendentals=0),
        compiler_params=pltpu.CompilerParams(vmem_limit_bytes=28 << 20),
        name="attend",
    )(position, *[near_core(t) for t in [*ready, *before]])


def project_kernel(group_size, quad, w_places, *refs):
    if quad:
        keep_in, recv_in = refs[:2]
        w_refs = refs[2:-4]
        send, keep, heads, w = refs[-4:]
        firsts, count = w_places()
        for (ref, col), at in zip(w_refs, firsts):
            w[pl.ds(pl.multiple_of(at, count), count), :] = ref[:, col : col + w.shape[1]]
        part = keep_in.shape[1]
        heads[:, :part] = keep_in[...]
        rows = send.shape[1]
        for s in range(group_size):
            heads[s * rows : (s + 1) * rows, part:] = recv_in[(s ^ 1) * rows : ((s ^ 1) + 1) * rows]
    else:
        heads, w, send = refs
    width = w.shape[1]
    step = min(width, 512)
    picks = send.shape[1]
    for at in range(0, width, step):
        out = jnp.dot(heads[...], w[:, at : at + step], preferred_element_type=F32)
        for s in range(group_size):
            piece = out[s * picks : (s + 1) * picks]
            if not quad:
                send[s, :, at : at + step] = piece.astype(BF16)
            elif s % 2:
                send[s // 2, :, at : at + step] = piece.astype(BF16)
            else:
                keep[s // 2, :, at : at + step] = piece


def project(group_size, quad, picks, heads, w_list, w_places, columns):
    start, width = columns

    def kernel(*refs):
        if not quad:
            return project_kernel(group_size, quad, w_places, *refs)
        views = [(ref, start if ref.shape[1] > width else 0) for ref in refs[2:-4]]
        return project_kernel(group_size, quad, w_places, *refs[:2], *views, *refs[-4:])

    scratch = []
    if quad:
        part = heads[0].shape[1]
        out = [jax.ShapeDtypeStruct((2, picks, width), BF16), jax.ShapeDtypeStruct((2, picks, width), F32)]
        scratch = [pltpu.VMEM((group_size * picks, 2 * part), BF16), pltpu.VMEM((2 * part, width), BF16)]
    else:
        out = [jax.ShapeDtypeStruct((group_size, picks, width), BF16)]
    return pl.pallas_call(
        kernel,
        out_shape=out,
        in_specs=[VMEM] * (len(heads) + len(w_list)),
        out_specs=[VMEM] * len(out),
        scratch_shapes=scratch,
        cost_estimate=pl.CostEstimate(flops=500_000_000, bytes_accessed=8_000_000, transcendentals=0),
        compiler_params=pltpu.CompilerParams(vmem_limit_bytes=20 << 20),
        name="project",
    )(*[near_core(t) for t in [*heads, *w_list]])


def layer(n_group, n_prompt, queries, fresh_latent, latent_cache, selected, position, latent_gain, kv_up, out_weight):
    picks = queries.shape[2]
    width = out_weight.shape[1]
    rows_kv = kv_up.shape[0]
    per = H // n_group
    quad = n_group == 4 and n_prompt == 8 and out_weight.shape[0] == 2 * DV
    m = DR // 2
    freqs = (10000.0 ** (-np.arange(m) / m)).astype(np.float32)
    freqs = jnp.asarray(np.tile(freqs, 4)[None, :])
    cache_t = jnp.swapaxes(latent_cache[0, 0], 0, 1)
    pieces, staged = cut(n_group, quad, kv_up, out_weight, [fresh_latent[0, 0], cache_t, queries[0, 0]])
    prepared = prep(n_group, quad, position, selected[0], latent_gain, freqs, *staged)
    blended = jnp.swapaxes(prepared[0], 0, 1)[None, None]

    if not quad:
        _, keysel, q_out = prepared
        kv_all = lax.all_gather(pieces[0], "prompt", axis=0)
        key_all = lax.all_gather(keysel, "group", axis=0)
        q_all = lax.all_to_all(q_out, "group", 0, 0)
        g = lax.axis_index("group")
        w_all = lax.all_gather(out_weight, "prompt", axis=0, tiled=True)
        w_own = lax.dynamic_index_in_dim(w_all.reshape(per, n_group, DV, width), g, 1, False)
        ins = [key_all[s] for s in range(n_group)] + [q_all[s] for s in range(n_group)]
        places = lambda: ([p * rows_kv for p in range(n_prompt)], rows_kv)
        ready = absorb(
            n_group, picks, ins + [kv_all[p] for p in range(n_prompt)], list(range(n_group)),
            [(n_group + s, 0) for s in range(n_group)], places,
        )
        heads = attend(n_group, quad, picks, position, ready, range(n_group), lambda s: s, [])
        (part,) = project(n_group, quad, picks, heads, [w_own.reshape(per * DV, width)], None, (0, width))
        got = lax.all_to_all(part, "group", 0, 0)
        attended = jnp.sum(got.astype(F32), 0).astype(BF16)
        return attended[None, None], blended

    _, far, near, own_q = prepared
    kv_own, w_own = pieces
    ny = 2
    nz = n_prompt // ny
    over_x = [(g, g ^ 2) for g in range(n_group)]
    over_core = [(g, g ^ 1) for g in range(n_group)]
    over_y = [(p, p ^ 1) for p in range(n_prompt)]
    up_z = lambda d: [(p, (p + d * ny) % n_prompt) for p in range(n_prompt)]

    def spread(own):
        column = [own] + [lax.ppermute(own, "prompt", up_z(k)) for k in (1, 3)]
        column.insert(2, lax.ppermute(column[1], "prompt", up_z(1)))
        return column + [lax.ppermute(t, "prompt", over_y) for t in column]

    kv = spread(kv_own)
    w = spread(w_own)
    far_in = lax.ppermute(far, "group", over_x)
    near_in = lax.ppermute(near, "group", over_core)
    cross_in = lax.ppermute(far_in, "group", over_core)

    def layers():
        z = lax.axis_index("prompt") // ny
        return [lax.rem(z + nz - k, nz) for k in range(nz)]

    def kv_places():
        y = lax.axis_index("prompt") % ny
        return [(z * ny + at) * rows_kv for at in (y, 1 - y) for z in layers()], rows_kv

    def w_places():
        y = lax.axis_index("prompt") % ny
        other = lax.rem(y + lax.axis_index("group"), 2)
        count = DV // 2
        return [(at * nz + z) * count for at in (other, 1 - other) for z in layers()], count

    slot_group = lambda s: lax.axis_index("group") ^ s
    q_rows = picks + picks // 2
    q_start = ROW + SELROWS
    ready = absorb(
        n_group, picks, [far, near_in, far_in, cross_in, own_q] + kv, [0, 1, 2, 3],
        [(4, 0), (1, q_start), (2, q_start + q_rows), (3, q_start)], kv_places,
    )
    heads = []
    for places in ((0,), (1, 2), (3,)):
        heads = attend(n_group, quad, picks, position, ready, places, slot_group, heads)
    keep, send = heads
    got = lax.ppermute(send, "group", over_core)
    out = []
    for i in range(2):
        columns = (i * width // 2, width // 2)
        mine, kept = project(n_group, quad, picks, [keep, got], w, w_places, columns)
        sums = kept + lax.ppermute(mine, "group", over_core).astype(F32)
        last = lax.ppermute(sums[1].astype(BF16), "group", over_x)
        out.append((sums[0] + last.astype(F32)).astype(BF16))
    attended = jnp.concatenate(out, 1)
    return attended[None, None], blended


def solution(mesh):
    in_specs = (
        P("prompt", "group", None, None),
        P("prompt", "group", None, None),
        P("prompt", "group", None, None),
        P("prompt", "group", None),
        P("prompt", None),
        P(),
        P("prompt", None),
        P("prompt", None),
    )
    out_specs = (P("prompt", "group", None, None), P("prompt", "group", None, None))
    body = functools.partial(layer, mesh.shape["group"], mesh.shape["prompt"])
    return jax.shard_map(body, mesh=mesh, in_specs=in_specs, out_specs=out_specs, check_vma=False)
```
